512 devices in a mesh: layer: 16 (over x, y_lo), feat: 32 (over z, y_hi, core).
Axes of the slice: x: 4, y: 8 (y_hi: 2, y_lo: 4; y = y_hi * 4 + y_lo), z: 8, core: 2. Of those that a mesh axis runs over, the one named last changes fastest.
Arguments:
- acts: bfloat16 [16, 1024, 8192], P(None, 'layer', 'feat'), may hold values from -6 to 6
- layer_order: int32 [16, 16], P('layer'), may hold values from 0 to 15, each once within a row
- groups: int32 [8192], P('feat'), may hold values from 0 to 63
- group_scale: float32 [16, 64], P('layer'), may hold values from 0.25 to 4
- shrink: float32 [16], P('layer'), may hold values from 0.1 to 0.6
Outputs:
- factor_tiles: float32 [16, 32, 16, 256, 256], P('layer', 'feat')
- far_tiles: float32 [16, 32, 128, 256], P('layer', 'feat')
The draws below stay inside these ranges and needn't reach their ends.
Inputs may be any that keep to these rules, and one draw needn't show every extreme that they name: Each row of layer_order names every layer once.
All inputs are finite; a program needn't handle non-finite values.
Results may differ from the reference program's by a relative error of at most 0.0003.
Values may be sent and summed in bfloat16 or wider, within the bound.
A program may use at most 64 MiB of HBM per device.

```python
import math
import jax
import jax.numpy as jnp
from jax import lax

D = 8192
TOK_DEV = 64
GROUPS = 64
LAYERS = 16
SOURCES = 16
TOKENS = 1024
PANELS = 32
PANEL = 256
HALF = 16


def touch_ends(result, rng, low, top_value):
    longest = result.shape.index(max(result.shape))
    spots = []
    for shift in (0, 1):
        where = [jax.random.randint(jax.random.fold_in(rng, axis), (), 0, length) for axis, length in enumerate(result.shape)]
        where[longest] = (where[longest] + shift) % result.shape[longest]
        spots.append(tuple(where))
    return result.at[spots[0]].set(low).at[spots[1]].set(top_value)


def level_of(rng, shape, pieces, least, high):
    level, own = 1.0, jax.random.fold_in(rng, 6)
    for dim, shards_of in pieces:
        heights = jnp.exp(jax.random.uniform(jax.random.fold_in(own, dim), (shards_of,), jnp.float32, least / len(pieces), high / len(pieces)))
        level = level * jnp.repeat(heights, shape[dim] // shards_of).reshape([-1 if axis == dim else 1 for axis in range(len(shape))])
    return level


def noise(own_key, shape, width, bound, shards=(), held_as=jnp.bfloat16):
    level = level_of(own_key, shape, shards, -0.22, 0.18) if shards else 1.0
    result = jax.random.normal(own_key, shape, jnp.float32) * width * level
    return jnp.minimum(jnp.maximum(result, -bound), bound).astype(held_as)


def setup_inputs(seed: int = 0) -> dict:
    arg_keys = jax.random.split(jax.random.key(seed), 6)
    return {
        "acts": noise(arg_keys[0], (LAYERS, TOKENS, D), 1.0, 6.0, ((1, 16), (2, 32))),
        "layer_order": jax.vmap(lambda own: jax.random.permutation(own, LAYERS))(jax.random.split(arg_keys[1], SOURCES)).reshape((SOURCES, LAYERS)).astype(jnp.int32),
        "groups": touch_ends(jax.random.randint(arg_keys[2], (D,), 0, GROUPS), jax.random.fold_in(arg_keys[2], 1), 0, GROUPS - 1).astype(jnp.int32),
        "group_scale": jnp.clip(jnp.exp(math.log(4.0) - 2.7725887 * jax.random.uniform(arg_keys[3], (LAYERS, GROUPS), jnp.float32) ** level_of(arg_keys[3], (LAYERS, GROUPS), ((0, 16),), -0.2, 0.2)), 0.25, 4.0),
        "shrink": jnp.clip(0.1 + 0.5 * jax.random.uniform(arg_keys[4], (LAYERS,), jnp.float32) ** level_of(arg_keys[4], (LAYERS,), ((0, 16),), -0.2, 0.2), 0.1, 0.6),
    }


def reference(acts, layer_order, groups, group_scale, shrink):
    sources = layer_order.shape[0]
    blocks = acts.reshape(LAYERS, sources, TOK_DEV, D)
    hits = (layer_order[:, None, :] == jnp.arange(LAYERS, dtype=jnp.int32)[None, :, None]).astype(jnp.int32)
    slot = jnp.sum(hits * jnp.arange(LAYERS, dtype=jnp.int32)[None, None, :], axis=2).astype(jnp.int32)
    source_ids = jnp.arange(sources, dtype=jnp.int32)[:, None]
    picked = blocks[slot, source_ids]
    by_layer = jnp.transpose(picked, (1, 0, 2, 3)).reshape(LAYERS, TOKENS, D)
    panel_ids = jnp.arange(PANELS, dtype=jnp.int32)
    offsets = jnp.arange(HALF, dtype=jnp.int32)
    columns = ((panel_ids[:, None] + offsets[None, :]) % PANELS).astype(jnp.int32)
    first = jnp.arange(HALF, dtype=jnp.int32)
    identity = jnp.eye(PANEL, dtype=jnp.float32)

    def one_layer(inputs):
        rows, gains, weight = inputs
        wide = rows.astype(jnp.float32)
        gram = jnp.dot(wide.T, wide, precision=lax.Precision.HIGHEST) / TOKENS
        mu = jnp.trace(gram) / D
        grid = gram.reshape(PANELS, PANEL, PANELS, PANEL).transpose(0, 2, 1, 3)
        tiles = grid[panel_ids[:, None], columns] * (1.0 - weight)
        diagonal = (weight * mu * gains[groups]).reshape(PANELS, PANEL)
        tiles = tiles.at[:, 0].add(diagonal[:, :, None] * identity[None])
        paired = grid[first, first + HALF]
        far = jnp.concatenate([paired[:, :PANEL // 2], paired[:, PANEL // 2:]], 0) * (1.0 - weight)
        return tiles, far

    factor_tiles, far_tiles = lax.map(one_layer, (by_layer, group_scale, shrink))
    return factor_tiles, far_tiles
```

```python
import jax
import jax.numpy as jnp
from jax import lax
from jax.experimental import pallas as pl
from jax.experimental.pallas import tpu as pltpu
from jax.sharding import PartitionSpec as P

X, YLO, YHI, Z, CORES = 4, 4, 2, 8, 2
BLOCKS = X * YLO
ROWS = 64
WIDTH = 256
TOKENS = BLOCKS * ROWS
FEATURES = WIDTH * Z * YHI * CORES
GROUPED = 4
CROSS_LAG = 2
ALL_HERE = 6
STEPS = 26
OFFSETS = [(dx, dy) for dy in (0, 1, 3, 2) for dx in (0, 1, 3, 2)]
F32 = jnp.float32


def product(left, right):
    return jnp.dot(left, right, preferred_element_type=F32)


def kernel(
    acts, order, groups, group_scale, shrink,
    out, far,
    outgoing, own, oth, sib, flipped, parts, sib_parts,
    a_send, a_recv, own_send, own_recv, cross_send, oth_send, oth_recv,
    sib_send, sib_recv, part_send, part_recv, partx_send, partx_recv, parts_send, parts_recv,
):
    layer = lax.axis_index("layer")
    feat = lax.axis_index("feat")
    x, ylo = layer // YLO, layer % YLO
    z, high, core = feat // (YHI * CORES), (feat // CORES) % YHI, feat % CORES

    def at(dz, other_high=False, other_core=False):
        zz = (z + dz + Z) % Z
        hh = 1 - high if other_high else high
        cc = 1 - core if other_core else core
        return (layer, zz * (YHI * CORES) + hh * CORES + cc)

    def peer(dx, dy):
        return (((x + dx) % X) * YLO + (ylo + dy) % YLO, feat)

    down, up, across, sibling = at(-1), at(1), at(0, True), at(0, False, True)

    def remote(src, dst, send, recv, device):
        return pltpu.make_async_remote_copy(
            src_ref=src, dst_ref=dst, send_sem=send, recv_sem=recv,
            device_id=device, device_id_type=pl.DeviceIdType.MESH,
        )

    barrier = pltpu.get_barrier_semaphore()
    partners = [peer(dx, dy) for dx, dy in OFFSETS[1:]] + [down, up, across, sibling]
    for device in partners:
        pl.semaphore_signal(
            barrier, inc=1, device_id=device, device_id_type=pl.DeviceIdType.MESH
        )

    def slot_of(target):
        slot = jnp.int32(0)
        for j in range(BLOCKS):
            slot = jnp.where(order[0, j] == target, j, slot)
        return slot

    for i, (dx, dy) in enumerate(OFFSETS):
        block = acts[slot_of(peer(dx, dy)[0])]
        if i == 0:
            own[0, 0] = block
        else:
            outgoing[i - 1] = block

    def clear(k, carry):
        out[k] = jnp.zeros((WIDTH, WIDTH), F32)
        return carry

    lax.fori_loop(0, 16, clear, 0)
    far[...] = jnp.zeros((WIDTH // 2, WIDTH), F32)
    pl.semaphore_wait(barrier, len(partners))

    scale = (1.0 - shrink[0]) * (1.0 / TOKENS)

    def landing(i):
        dx, dy = OFFSETS[i]
        return OFFSETS.index(((-dx) % X, (-dy) % YLO))

    def first_copy(i):
        to = landing(i)
        return remote(
            outgoing.at[i - 1], own.at[0, to], a_send, a_recv.at[to], peer(*OFFSETS[i])
        )

    for i in range(1, BLOCKS):
        first_copy(i).start()

    def first_arrival(b):
        remote(own.at[0, b], own.at[0, b], a_send, a_recv.at[b], sibling).wait_recv()

    def grouped(ref, slot, q):
        return ref[slot, pl.ds(q * GROUPED, GROUPED)].reshape(GROUPED * ROWS, WIDTH)

    def flipped_group(q):
        return flipped[:, pl.ds(pl.multiple_of(q * GROUPED * ROWS, GROUPED * ROWS), GROUPED * ROWS)]

    def finished(total, q):
        return total * jnp.where(q == BLOCKS // GROUPED - 1, scale, 1.0)

    def accumulate(k, panel, q):
        out[k] = finished(out[k] + product(flipped_group(q), panel), q)

    lower = z < Z // 2

    def accumulate_far(q):
        mine, opposite = grouped(own, 0, q), grouped(own, 4, q)
        half = WIDTH // 2
        left = jnp.where(lower, mine[:, :half], opposite[:, half:])
        right = jnp.where(lower, opposite, mine)
        term = lax.dot_general(
            left, right, (((0,), (0,)), ((), ())), preferred_element_type=F32
        )
        far[...] = finished(far[...] + term, q)

    def to_sibling(ref, slot, place, q):
        part = pl.ds(q * GROUPED, GROUPED)
        remote(
            ref.at[slot, part], sib.at[place, part], sib_send, sib_recv.at[place, q], sibling
        ).start()

    def inside(b):
        return (b >= 0) & (b < BLOCKS)

    def ends_group(b):
        return inside(b) & (b % GROUPED == GROUPED - 1)

    def step(t, carry):
        @pl.when(t < BLOCKS)
        def _():
            @pl.when((t > 0) & (t <= ALL_HERE))
            def _():
                first_arrival(t)

            remote(
                own.at[0, t], own.at[1, t], own_send, own_recv.at[1, t], down
            ).start()

        for d in range(1, 5):
            b = t - d

            @pl.when(inside(b))
            def _(d=d, b=b):
                remote(
                    own.at[d, b], own.at[d, b], own_send, own_recv.at[d, b], down
                ).wait_recv()
                if d < 4:
                    remote(
                        own.at[d, b], own.at[d + 1, b], own_send, own_recv.at[d + 1, b], down
                    ).start()
                if d >= 3:
                    @pl.when(high == 4 - d)
                    def _():
                        remote(
                            own.at[d, b], oth.at[0, b], cross_send, oth_recv.at[0, b], across
                        ).start()

        first = 3 + high + CROSS_LAG
        for o in range(4):
            b = t - first - o

            @pl.when(inside(b))
            def _(o=o, b=b):
                remote(
                    oth.at[o, b], oth.at[o, b], oth_send, oth_recv.at[o, b], up
                ).wait_recv()
                if o < 3:
                    remote(
                        oth.at[o, b], oth.at[o + 1, b], oth_send, oth_recv.at[o + 1, b], up
                    ).start()

        for d in range(5):
            b = t - d
            place = d - 1 + core

            @pl.when(ends_group(b) & (place >= 0) & (place < 4))
            def _(d=d, b=b, place=place):
                to_sibling(own, d, place, b // GROUPED)

        for o in range(4):
            b = t - first - o

            @pl.when(ends_group(b))
            def _(o=o, b=b):
                to_sibling(oth, o, 4 + o, b // GROUPED)

        @pl.when(t == ALL_HERE)
        def _():
            for b in range(ALL_HERE + 1, BLOCKS):
                first_arrival(b)

            def add(b, total):
                values = own[0, b].astype(F32)
                squares = (values * values).reshape(ROWS // 8, 8, WIDTH).sum(axis=0)
                return total + squares[:, :128] + squares[:, 128:]

            parts[0, 0] = lax.fori_loop(0, BLOCKS, add, jnp.zeros((8, 128), F32))

        ring = t - (ALL_HERE + 1)

        @pl.when((ring >= 1) & (ring < Z))
        def _():
            remote(
                parts.at[0, ring], parts.at[0, ring], part_send, part_recv.at[ring], down
            ).wait_recv()

        @pl.when((ring >= 0) & (ring < Z - 1))
        def _():
            remote(
                parts.at[0, ring], parts.at[0, ring + 1], part_send, part_recv.at[ring + 1], down
            ).start()

        crossing = remote(parts.at[0], parts.at[1], partx_send, partx_recv, across)
        sharing = remote(parts, sib_parts, parts_send, parts_recv, sibling)

        @pl.when(ring == Z - 1)
        def _():
            crossing.start()

        @pl.when(ring == Z + 1)
        def _():
            crossing.wait()
            sharing.start()

        @pl.when(ring == Z + 2)
        def _():
            sharing.wait()
            trace = jnp.sum(parts[...]) + jnp.sum(sib_parts[...])
            mu = trace * (1.0 / TOKENS / FEATURES)

            def gain_of(g, gains):
                return jnp.where(groups[...] == g, group_scale[0, g], gains)

            gains = lax.fori_loop(
                0, group_scale.shape[1], gain_of, jnp.zeros((1, WIDTH), F32)
            )
            rows = lax.broadcasted_iota(jnp.int32, (WIDTH, WIDTH), 0)
            columns = lax.broadcasted_iota(jnp.int32, (WIDTH, WIDTH), 1)
            out[0] = out[0] + jnp.where(rows == columns, shrink[0] * mu * gains, 0.0)

        @pl.when((t < BLOCKS) & (t % GROUPED == GROUPED - 1))
        def _():
            q = t // GROUPED
            panel = grouped(own, 0, q)
            flipped[:, pl.ds(pl.multiple_of(q * GROUPED * ROWS, GROUPED * ROWS), GROUPED * ROWS)] = panel.T
            accumulate(0, panel, q)

        for d in range(1, 5):
            b = t - d

            @pl.when(ends_group(b))
            def _(d=d, b=b):
                q = b // GROUPED
                if d < 4:
                    accumulate(4 * d, grouped(own, d, q), q)
                else:
                    accumulate_far(q)

        for o in range(4):
            b = t - first - o

            @pl.when(ends_group(b))
            def _(o=o, b=b):
                q = b // GROUPED
                accumulate(14 - 4 * o, grouped(oth, o, q), q)

        for place in range(8):
            if place < 4:
                b = t - 1 - (place + core)
                k = 4 * place + 1 + 2 * core
            else:
                b = t - 1 - first - (place - 4)
                k = 15 - 4 * (place - 4) - 2 * core

            @pl.when(ends_group(b))
            def _(place=place, b=b, k=k):
                q = b // GROUPED
                part = pl.ds(q * GROUPED, GROUPED)
                remote(
                    sib.at[place, part], sib.at[place, part], sib_send,
                    sib_recv.at[place, q], sibling,
                ).wait_recv()
                accumulate(k, grouped(sib, place, q), q)

        return carry

    lax.fori_loop(0, STEPS, step, 0)

    def sent(ref, sem):
        remote(ref, ref, sem, sem, sibling).wait_send()

    sent(outgoing, a_send)
    sent(own.at[pl.ds(0, 4)], own_send)
    sent(oth.at[0], cross_send)
    sent(oth.at[pl.ds(0, 3)], oth_send)
    sent(sib, sib_send)
    sent(parts.at[0, pl.ds(0, Z - 1)], part_send)


def shards(acts, layer_order, groups, group_scale, shrink):
    vmem = pl.BlockSpec(memory_space=pltpu.VMEM)
    smem = pl.BlockSpec(memory_space=pltpu.SMEM)
    dma = pltpu.SemaphoreType.DMA
    bf16 = jnp.bfloat16
    factor, far = pl.pallas_call(
        kernel,
        out_shape=(
            jax.ShapeDtypeStruct((16, WIDTH, WIDTH), F32),
            jax.ShapeDtypeStruct((WIDTH // 2, WIDTH), F32),
        ),
        in_specs=[vmem, smem, vmem, smem, smem],
        out_specs=(vmem, vmem),
        scratch_shapes=[
            pltpu.VMEM((BLOCKS - 1, ROWS, WIDTH), bf16),
            pltpu.VMEM((5, BLOCKS, ROWS, WIDTH), bf16),
            pltpu.VMEM((4, BLOCKS, ROWS, WIDTH), bf16),
            pltpu.VMEM((8, BLOCKS, ROWS, WIDTH), bf16),
            pltpu.VMEM((WIDTH, TOKENS), bf16),
            pltpu.VMEM((2, Z, 8, 128), F32),
            pltpu.VMEM((2, Z, 8, 128), F32),
            dma, dma((BLOCKS,)), dma, dma((5, BLOCKS)), dma, dma, dma((4, BLOCKS)),
            dma, dma((8, BLOCKS // GROUPED)), dma, dma((Z,)), dma, dma, dma, dma,
        ],
        compiler_params=pltpu.CompilerParams(
            collective_id=0, has_side_effects=True, vmem_limit_bytes=40 * 1024 * 1024
        ),
        name="gram",
    )(acts, layer_order, groups[None, :], group_scale, shrink)
    return (factor[None, None], far[None, None])


def solution(mesh):
    placed = (P(None, "layer", "feat"), P("layer", None), P("feat"), P("layer", None), P("layer"))
    return jax.shard_map(
        shards,
        mesh=mesh,
        in_specs=placed,
        out_specs=(P("layer", "feat", None, None, None), P("layer", "feat", None, None)),
        check_vma=False,
    )
```
